512 devices in a mesh: gx: 8 (over y, core), gy: 16 (over z), lev: 4 (over x).
Axes of the slice: x: 4, y: 4, z: 16, core: 2. Of those that a mesh axis runs over, the one named last changes fastest.
Arguments:
- state: bfloat16 [1024, 128, 8, 512], P('gx', 'gy', 'lev'), may hold values from -6 to 6
- obs_col: int32 [4096], P('gx'), may hold values from 0 to 127
- obs_row: int32 [4096], P('gx'), may hold values from 0 to 127
- foot_off: int32 [4096, 8], P('gx'), may hold values from 0 to 84
- obs_lev: int32 [4096], P('gx'), may hold values from 0 to 7
- obs_val: float32 [4096], P('gx'), may hold values from -6 to 6
- obs_err: float32 [4096], P('gx'), may hold values from 0.5 to 2
- loc: bfloat16 [1024, 128, 512], P('gx', ('gy', 'lev')), may hold values from 0.099609375 to 1
Outputs:
- mean_out: float32 [1024, 128, 8], P('gx', ('gy', 'lev'))
- anom_out: bfloat16 [1024, 128, 8, 512], P('gx', ('gy', 'lev'))
The draws below stay inside these ranges and needn't reach their ends.
All inputs are finite; a program needn't handle non-finite values.
Results may differ from the reference program's by a relative error of at most 0.009.
Values may be sent and summed in bfloat16 or wider, within the bound.
No kernel may reach another device: no remote copies, remote signals or barrier semaphores. Data moves between devices by JAX's collectives and lax.ppermute only.
A program may use at most 64 MiB of HBM per device.

```python
import math
import jax
import jax.numpy as jnp
from jax import lax

M = 512
CXD = 128
LEV = 8
NOBS = 512
KF = 8
HW = 8
DY = 2
NX = 1024
NY = 128
OBS_ALL = 4096
N_GX = 8


def place_ends(entries, key, smallest, high):
    extent = entries.shape
    spot = [jax.random.randint(jax.random.fold_in(key, axis), (), 0, extent[axis]) for axis in range(len(extent))]
    entries = entries.at[tuple(spot)].set(smallest)
    longest = extent.index(max(extent))
    spot[longest] = (spot[longest] + 1) % extent[longest]
    return entries.at[tuple(spot)].set(high)


def block_levels(own_key, dims, pieces, smallest, top_value):
    level, own = 1.0, jax.random.fold_in(own_key, 6)
    for dim, parts in pieces:
        draws = jnp.exp(jax.random.uniform(jax.random.fold_in(own, dim), (parts,), jnp.float32, smallest / len(pieces), top_value / len(pieces)))
        level = level * jnp.repeat(draws, dims[dim] // parts).reshape([-1 if axis == dim else 1 for axis in range(len(dims))])
    return level


def gaussian(own_key, dims, deviation, most, shards=(), kind=jnp.bfloat16):
    level = block_levels(own_key, dims, shards, -0.22, 0.18) if shards else 1.0
    array = jax.random.normal(own_key, dims, jnp.float32) * deviation * level
    return jnp.minimum(jnp.maximum(array, -most), most).astype(kind)


def setup_inputs(seed: int = 0) -> dict:
    key_of = jax.random.split(jax.random.key(seed), 9)
    return {
        "state": gaussian(key_of[0], (NX, NY, LEV, M), 1.0, 6.0, ((0, 8), (1, 16), (2, 4))),
        "obs_col": place_ends(jax.random.randint(key_of[1], (OBS_ALL,), 0, CXD), jax.random.fold_in(key_of[1], 1), 0, CXD - 1).astype(jnp.int32),
        "obs_row": place_ends(jax.random.randint(key_of[2], (OBS_ALL,), 0, NY), jax.random.fold_in(key_of[2], 1), 0, NY - 1).astype(jnp.int32),
        "foot_off": place_ends(jax.random.randint(key_of[3], (OBS_ALL, KF), 0, (2 * HW + 1) * (2 * DY + 1)), jax.random.fold_in(key_of[3], 1), 0, ((2 * HW + 1) * (2 * DY + 1)) - 1).astype(jnp.int32),
        "obs_lev": place_ends(jax.random.randint(key_of[4], (OBS_ALL,), 0, LEV), jax.random.fold_in(key_of[4], 1), 0, LEV - 1).astype(jnp.int32),
        "obs_val": gaussian(key_of[5], (OBS_ALL,), 1.0, 6.0, ((0, 8),), jnp.float32),
        "obs_err": jnp.clip(jnp.exp(math.log(2.0) - 1.3862944 * jax.random.uniform(key_of[6], (OBS_ALL,), jnp.float32) ** block_levels(key_of[6], (OBS_ALL,), ((0, 8),), -0.2, 0.2)), 0.5, 2.0),
        "loc": jnp.clip(0.099609375 + 0.9003906 * jax.random.uniform(key_of[7], (NX, NY, NOBS), jnp.float32) ** block_levels(key_of[7], (NX, NY, NOBS), ((0, 8), (1, 64)), -0.2, 0.2), 0.099609375, 1.0).astype(jnp.bfloat16),
    }


def footprint(obs_col, obs_row, foot_off):
    span = 2 * DY + 1
    shift_x = foot_off // span - HW
    shift_y = foot_off % span - DY
    x_ext = obs_col[:, None] + shift_x + HW
    y_glob = jnp.clip(obs_row[:, None] + shift_y, 0, NY - 1)
    return (x_ext.astype(jnp.int32), y_glob.astype(jnp.int32))

def analyse(block, weight, hx_sum, values, errors):
    members = block.shape[-1]
    hbar = lax.optimization_barrier(jnp.mean(hx_sum, axis=1))
    yanom = hx_sum - hbar[:, None]
    innov = values - hbar
    cov = jnp.dot(yanom, yanom.T, precision=lax.Precision.HIGHEST) / (members - 1) + jnp.diag(errors)
    chol = jnp.linalg.cholesky(cov)
    root = chol + jnp.diag(jnp.sqrt(errors))
    first = lax.linalg.triangular_solve(chol, innov[:, None], left_side=True, lower=True)
    scaled = lax.linalg.triangular_solve(root, yanom, left_side=True, lower=True)
    wvec = lax.linalg.triangular_solve(chol, first, left_side=True, lower=True, transpose_a=True)[:, 0]
    zmat = lax.linalg.triangular_solve(chol, scaled, left_side=True, lower=True, transpose_a=True).astype(jnp.bfloat16)
    xbar = lax.optimization_barrier(jnp.mean(block, axis=-1, dtype=jnp.float32))
    anom = (block.astype(jnp.float32) - xbar[..., None]).astype(jnp.bfloat16)
    flat = anom.reshape(-1, members)
    cross = jnp.dot(flat.astype(jnp.float32), yanom.astype(jnp.bfloat16).T.astype(jnp.float32), preferred_element_type=jnp.float32) / (members - 1)
    n_obs = hx_sum.shape[0]
    gain = (cross.reshape(block.shape[:-1] + (n_obs,)) * weight[:, :, None, :].astype(jnp.float32)).astype(jnp.bfloat16)
    mean_part = xbar + lax.optimization_barrier(jnp.sum(gain.astype(jnp.float32) * wvec, axis=-1))
    update = jnp.dot(gain.reshape(-1, n_obs).astype(jnp.float32), zmat.astype(jnp.float32), preferred_element_type=jnp.float32)
    anom_part = (flat.astype(jnp.float32) - update).astype(jnp.bfloat16).reshape(block.shape)
    return (mean_part, anom_part)

def reference(state, obs_col, obs_row, foot_off, obs_lev, obs_val, obs_err, loc):

    def one_tile(inputs):
        index, cols, rows, offsets, levels, values, errors = inputs
        x_ext, y_glob = footprint(cols, rows, offsets)
        x_glob = ((index * CXD + x_ext - HW) % NX).astype(jnp.int32)
        picked = state[x_glob, y_glob, levels[:, None].astype(jnp.int32), :]
        hx_sum = lax.optimization_barrier(jnp.sum(picked.astype(jnp.float32), axis=1)) / KF
        block = lax.dynamic_slice_in_dim(state, (index * CXD).astype(jnp.int32), CXD, 0)
        weight = lax.dynamic_slice_in_dim(loc, (index * CXD).astype(jnp.int32), CXD, 0)
        return analyse(block, weight, hx_sum, values, errors)
    tiles = (jnp.arange(N_GX, dtype=jnp.int32), obs_col.reshape(N_GX, NOBS), obs_row.reshape(N_GX, NOBS), foot_off.reshape(N_GX, NOBS, KF), obs_lev.reshape(N_GX, NOBS), obs_val.reshape(N_GX, NOBS), obs_err.reshape(N_GX, NOBS))
    means, anoms = lax.map(one_tile, tiles)
    return (means.reshape(NX, NY, LEV), anoms.reshape(NX, NY, LEV, M))
```

```python
import jax, jax.numpy as jnp
from jax import lax
from jax.experimental import pallas as pl
from jax.experimental.pallas import tpu as pltpu
from jax.sharding import PartitionSpec as P

KF = 8
HW = 8
DY = 2
F32=jnp.float32
BF=jnp.bfloat16
HI=lax.Precision.HIGHEST
SUB=32
SUP=128

def mm(a,b,dims,prec=HI):
    return lax.dot_general(a,b,(dims,((),())),precision=prec,preferred_element_type=F32)
def mm3(a,b):
    hi=a.astype(BF)
    rest=a-hi.astype(F32)
    mid=rest.astype(BF)
    low=(rest-mid.astype(F32)).astype(BF)
    return mm(hi,b,NN,None)+(mm(mid,b,NN,None)+mm(low,b,NN,None))
NN=((1,),(0,)); NT=((1,),(1,)); TN=((0,),(0,))

def factor_block(R, off, sq):
    nv=SUB//8
    row=lax.broadcasted_iota(jnp.int32,(8,128),0)
    lane=lax.broadcasted_iota(jnp.int32,(8,128),1)
    C=[[jnp.broadcast_to(R[8*v:8*v+8, off+j:off+j+1],(8,128)) if v>=j//8 else None for v in range(nv)] for j in range(SUB)]
    X=[jnp.where(lane==row+8*v,1.0,0.0).astype(F32) for v in range(nv)]
    G=list(X)
    rs=[jnp.zeros((8,128),F32) for _ in range(nv)]
    def rowb(t,i):
        return jnp.broadcast_to(t[i:i+1,:],(8,128))
    for j in range(SUB):
        vj,ij=divmod(j,8)
        p=rowb(C[j][vj],ij)
        inv=1.0/p
        col=[C[j][v] if v>=vj else None for v in range(nv)]
        q=[None if c is None else c*inv for c in col]
        for k in range(j+1,SUB):
            vk,ik=divmod(k,8)
            ck=rowb(col[vk],ik)
            for v in range(vk,nv):
                C[k][v]=C[k][v]-q[v]*ck
        r=lax.rsqrt(p)
        below=row>ij
        qm=[None if t is None else t for t in q]
        qm[vj]=jnp.where(below,q[vj],0.0)
        rs[vj]=jnp.where(row==ij,r,rs[vj])
        sp=p*r
        xj=rowb(X[vj],ij)
        g=1.0/(sp+rowb(sq[vj],ij))
        gj=rowb(G[vj],ij)*g
        G[vj]=jnp.where(row==ij,gj,G[vj])
        gs=gj*sp
        for v in range(vj,nv):
            X[v]=X[v]-qm[v]*xj
            G[v]=G[v]-qm[v]*gs
    X=[X[v]*rs[v] for v in range(nv)]
    return jnp.concatenate(X,0)[:,:SUB], jnp.concatenate(G,0)[:,:SUB]

def solve_kernel(y_ref, innov_ref, errr_ref, errc_ref, z_ref, w_ref, A, U, Li, Gi):
    n=A.shape[0]
    M=y_ref.shape[1]
    y=y_ref[...]
    A[...]=mm(y,y,NT,None)*(1.0/(M-1))
    Li[...]=jnp.zeros_like(Li)
    Gi[...]=jnp.zeros_like(Gi)
    sup=n//SUP
    ii=lax.broadcasted_iota(jnp.int32,(SUP,SUP),0)
    jj=lax.broadcasted_iota(jnp.int32,(SUP,SUP),1)
    for s in range(sup):
        w0=s*SUP
        A[w0:w0+SUP,w0:w0+SUP]=A[w0:w0+SUP,w0:w0+SUP]+jnp.where(ii==jj,errr_ref[:,w0:w0+SUP],0.0)
    for s in range(sup):
        w0=s*SUP
        for t in range(SUP//SUB):
            k0=w0+t*SUB
            R=A[k0:k0+SUB,w0:n]
            if t:
                R=R-mm(U[w0:k0,k0:k0+SUB],U[w0:k0,w0:n],TN)
            sq=jnp.broadcast_to(jnp.sqrt(errc_ref[k0:k0+SUB,:]),(SUB,128))
            sq=[sq[8*v:8*v+8] for v in range(SUB//8)]
            x,g=factor_block(R,t*SUB,sq)
            U[k0:k0+SUB,w0:n]=mm(x,R,NN)
            Li[k0:k0+SUB,k0:k0+SUB]=x
            Gi[k0:k0+SUB,k0:k0+SUB]=g
        w1=w0+SUP
        if w1<n:
            A[w1:n,w1:n]=A[w1:n,w1:n]-mm(U[w0:w1,w1:n],U[w0:w1,w1:n],TN)
    for s in range(sup):
        w0=s*SUP
        L=U[w0:w0+SUP,w0:w0+SUP].T
        for B in (Li,Gi):
            T=B[w0:w0+SUP,w0:w0+SUP]
            size=SUB
            while size<SUP:
                mask=((ii//(2*size))==(jj//(2*size)))&((ii//size)>(jj//size))
                N=jnp.where(mask,L,0.0)
                T=T-mm(T,mm(N,T,NN),NN)
                size*=2
            B[w0:w0+SUP,w0:w0+SUP]=T
    size=SUP
    while size<n:
        for a0 in range(0,n,2*size):
            b0=a0+size; b1=b0+size
            for B in (Li,Gi):
                t=mm(U[a0:b0,b0:b1],B[a0:b0,a0:b0],TN)
                B[b0:b1,a0:b0]=-mm(B[b0:b1,b0:b1],t,NN)
        size*=2
    S=jnp.concatenate([mm3(Gi[s*SUP:(s+1)*SUP,:(s+1)*SUP],y_ref[:(s+1)*SUP,:]) for s in range(sup)],0)
    v=jnp.sum(Li[...]*innov_ref[...],axis=1,keepdims=True)
    w_ref[...]=jnp.sum(Li[...]*v,axis=0,keepdims=True)
    for s in range(sup):
        z_ref[s*SUP:(s+1)*SUP,:]=mm(Li[s*SUP:,s*SUP:(s+1)*SUP],S[s*SUP:],TN).astype(z_ref.dtype)

def solve(y, innov, err):
    n,M=y.shape
    return pl.pallas_call(solve_kernel,
        out_shape=(jax.ShapeDtypeStruct((n,M),BF),jax.ShapeDtypeStruct((1,n),F32)),
        in_specs=[pl.BlockSpec(memory_space=pltpu.VMEM)]*4,
        out_specs=(pl.BlockSpec(memory_space=pltpu.VMEM),)*2,
        scratch_shapes=[pltpu.VMEM((n,n),F32)]*4,
        compiler_params=pltpu.CompilerParams(vmem_limit_bytes=40<<20),
        cost_estimate=pl.CostEstimate(flops=6*10**9,bytes_accessed=2<<20,transcendentals=0),
    )(y, innov[None,:], err[None,:], err[:,None])


def split3(x):
    hi = lax.reduce_precision(x, 8, 7)
    mid = lax.reduce_precision(x - hi, 8, 7)
    return hi, mid, x - hi - mid


def pack(anom, mean):
    cols = jnp.stack(split3(mean), axis=-1)
    cols = jnp.pad(cols, [(0, 0)] * (cols.ndim - 1) + [(0, 125)])
    return jnp.concatenate([anom, cols], axis=-1).astype(BF)


def unpack_sum(parts, members):
    total = jnp.sum(parts.astype(F32), axis=0)
    return total[..., :members], jnp.sum(total[..., members:], axis=-1)


def swap(array, axis):
    return lax.all_to_all(array, axis, split_axis=0, concat_axis=0, tiled=True)


def halo(state, axis):
    size = lax.axis_size(axis)
    up = [(i, (i + 1) % size) for i in range(size)]
    down = [(j, i) for i, j in up]
    before = lax.ppermute(state[state.shape[0] - HW :], axis, up)
    after = lax.ppermute(state[:HW], axis, down)
    return before, after


def observe(state, obs_col, obs_row, foot_off, obs_lev, ny_total):
    nx, ny, nl, members = state.shape
    span = 2 * DY + 1
    x_ext = obs_col[:, None] + foot_off // span
    y = jnp.clip(obs_row[:, None] + foot_off % span - DY, 0, ny_total - 1) - lax.axis_index("gy") * ny
    lv = obs_lev[:, None] - lax.axis_index("lev") * nl
    inside = (y >= 0) & (y < ny) & (lv >= 0) & (lv < nl)
    code = jnp.where(inside, (x_ext * ny + y) * nl + lv, -1)
    width = (nx + 2 * HW) * ny * nl
    edge = HW * ny * nl
    col = jnp.arange(width, dtype=jnp.int32)[None, :]
    hits = jnp.zeros((code.shape[0], width), F32)
    for slot in range(code.shape[1]):
        hits = hits + (code[:, slot, None] == col).astype(F32)
    select = hits.astype(BF)
    before, after = halo(state, "gx")
    total = jnp.dot(select[:, edge : width - edge], state.reshape(-1, members), preferred_element_type=F32)
    total = total + jnp.dot(select[:, :edge], before.reshape(-1, members), preferred_element_type=F32)
    total = total + jnp.dot(select[:, width - edge :], after.reshape(-1, members), preferred_element_type=F32)
    return total / KF


def share(part):
    n_obs, members = part.shape
    mean = jnp.mean(part, axis=1)
    msg = pack(part - mean[:, None], mean)
    for axis in ("lev", "gy"):
        size = lax.axis_size(axis)
        got = swap(msg.reshape(size, msg.shape[0] // size, msg.shape[1]), axis)
        msg = pack(*unpack_sum(got, members))
    size = lax.axis_size("gy")
    msg = swap(jnp.broadcast_to(msg[None], (size,) + msg.shape), "gy").reshape(-1, msg.shape[1])
    msg = lax.all_gather(msg, "lev", axis=0, tiled=True)
    return msg[:, :members], jnp.sum(msg[:, members : members + 3].astype(F32), axis=1)


def relay(state):
    nx, ny, nl, members = state.shape
    size = lax.axis_size("lev")
    parts = jnp.moveaxis(state.reshape(nx, size, ny // size, nl, members), 1, 0)
    got = swap(parts, "lev")
    return jnp.moveaxis(got, 0, 2).reshape(nx, ny // size, size * nl, members)


def local(state, obs_col, obs_row, foot_off, obs_lev, obs_val, obs_err, loc):
    members = state.shape[-1]
    ny_total = state.shape[1] * lax.axis_size("gy")
    part = observe(state, obs_col, obs_row, foot_off, obs_lev, ny_total)
    ybf, hbar = share(part)
    state, ybf, hbar = lax.optimization_barrier((state, ybf, hbar))
    block = relay(state)
    zmat, wrow = solve(ybf, obs_val - hbar, obs_err)
    n_obs = zmat.shape[0]
    xbar = jnp.mean(block, axis=-1, dtype=F32)
    anom = (block.astype(F32) - xbar[..., None]).astype(BF)
    flat = anom.reshape(-1, members)
    cross = jnp.dot(flat, ybf.T, preferred_element_type=F32) / (members - 1)
    gain = (cross.reshape(block.shape[:-1] + (n_obs,)) * loc[:, :, None, :].astype(F32)).astype(BF)
    mean_part = xbar + jnp.sum(gain.astype(F32) * wrow[0], axis=-1)
    update = jnp.dot(gain.reshape(-1, n_obs), zmat, preferred_element_type=F32)
    anom_part = (flat.astype(F32) - update).astype(BF).reshape(block.shape)
    return (mean_part, anom_part)


def solution(mesh):
    return jax.shard_map(
        local,
        mesh=mesh,
        in_specs=(
            P("gx", "gy", "lev", None),
            P("gx"),
            P("gx"),
            P("gx", None),
            P("gx"),
            P("gx"),
            P("gx"),
            P("gx", ("gy", "lev"), None),
        ),
        out_specs=(P("gx", ("gy", "lev"), None), P("gx", ("gy", "lev"), None, None)),
        check_vma=False,
    )
```

```python
import functools

import jax, jax.numpy as jnp
from jax import lax
from jax.experimental import pallas as pl
from jax.experimental.pallas import tpu as pltpu
from jax.sharding import PartitionSpec as P

KF = 8
HW = 8
DY = 2
F32=jnp.float32
BF=jnp.bfloat16
HI=lax.Precision.HIGHEST
SUB=32
SUP=128

def mm(a,b,dims,prec=HI):
    return lax.dot_general(a,b,(dims,((),())),precision=prec,preferred_element_type=F32)
def mm3(a,b):
    hi=a.astype(BF)
    rest=a-hi.astype(F32)
    mid=rest.astype(BF)
    low=(rest-mid.astype(F32)).astype(BF)
    return mm(hi,b,NN,None)+(mm(mid,b,NN,None)+mm(low,b,NN,None))
NN=((1,),(0,)); NT=((1,),(1,)); TN=((0,),(0,))

def factor_block(R, off, sq):
    nv=SUB//8
    row=lax.broadcasted_iota(jnp.int32,(8,128),0)
    lane=lax.broadcasted_iota(jnp.int32,(8,128),1)
    C=[[jnp.broadcast_to(R[8*v:8*v+8, off+j:off+j+1],(8,128)) if v>=j//8 else None for v in range(nv)] for j in range(SUB)]
    X=[jnp.where(lane==row+8*v,1.0,0.0).astype(F32) for v in range(nv)]
    G=list(X)
    rs=[jnp.zeros((8,128),F32) for _ in range(nv)]
    def rowb(t,i):
        return jnp.broadcast_to(t[i:i+1,:],(8,128))
    for j in range(SUB):
        vj,ij=divmod(j,8)
        p=rowb(C[j][vj],ij)
        inv=1.0/p
        col=[C[j][v] if v>=vj else None for v in range(nv)]
        q=[None if c is None else c*inv for c in col]
        for k in range(j+1,SUB):
            vk,ik=divmod(k,8)
            ck=rowb(col[vk],ik)
            for v in range(vk,nv):
                C[k][v]=C[k][v]-q[v]*ck
        r=lax.rsqrt(p)
        below=row>ij
        qm=[None if t is None else t for t in q]
        qm[vj]=jnp.where(below,q[vj],0.0)
        rs[vj]=jnp.where(row==ij,r,rs[vj])
        sp=p*r
        xj=rowb(X[vj],ij)
        g=1.0/(sp+rowb(sq[vj],ij))
        gj=rowb(G[vj],ij)*g
        G[vj]=jnp.where(row==ij,gj,G[vj])
        gs=gj*sp
        for v in range(vj,nv):
            X[v]=X[v]-qm[v]*xj
            G[v]=G[v]-qm[v]*gs
    X=[X[v]*rs[v] for v in range(nv)]
    return jnp.concatenate(X,0)[:,:SUB], jnp.concatenate(G,0)[:,:SUB]

def solve_kernel(y_ref, innov_ref, errr_ref, errc_ref, z_ref, w_ref, A, U, Li, Gi):
    n=A.shape[0]
    M=y_ref.shape[1]
    y=y_ref[...]
    A[...]=mm(y,y,NT,None)*(1.0/(M-1))
    Li[...]=jnp.zeros_like(Li)
    Gi[...]=jnp.zeros_like(Gi)
    sup=n//SUP
    ii=lax.broadcasted_iota(jnp.int32,(SUP,SUP),0)
    jj=lax.broadcasted_iota(jnp.int32,(SUP,SUP),1)
    for s in range(sup):
        w0=s*SUP
        A[w0:w0+SUP,w0:w0+SUP]=A[w0:w0+SUP,w0:w0+SUP]+jnp.where(ii==jj,errr_ref[:,w0:w0+SUP],0.0)
    for s in range(sup):
        w0=s*SUP
        for t in range(SUP//SUB):
            k0=w0+t*SUB
            R=A[k0:k0+SUB,w0:n]
            if t:
                R=R-mm(U[w0:k0,k0:k0+SUB],U[w0:k0,w0:n],TN)
            sq=jnp.broadcast_to(jnp.sqrt(errc_ref[k0:k0+SUB,:]),(SUB,128))
            sq=[sq[8*v:8*v+8] for v in range(SUB//8)]
            x,g=factor_block(R,t*SUB,sq)
            U[k0:k0+SUB,w0:n]=mm(x,R,NN)
            Li[k0:k0+SUB,k0:k0+SUB]=x
            Gi[k0:k0+SUB,k0:k0+SUB]=g
        w1=w0+SUP
        if w1<n:
            A[w1:n,w1:n]=A[w1:n,w1:n]-mm(U[w0:w1,w1:n],U[w0:w1,w1:n],TN)
    for s in range(sup):
        w0=s*SUP
        L=U[w0:w0+SUP,w0:w0+SUP].T
        for B in (Li,Gi):
            T=B[w0:w0+SUP,w0:w0+SUP]
            size=SUB
            while size<SUP:
                mask=((ii//(2*size))==(jj//(2*size)))&((ii//size)>(jj//size))
                N=jnp.where(mask,L,0.0)
                T=T-mm(T,mm(N,T,NN),NN)
                size*=2
            B[w0:w0+SUP,w0:w0+SUP]=T
    size=SUP
    while size<n:
        for a0 in range(0,n,2*size):
            b0=a0+size; b1=b0+size
            for B in (Li,Gi):
                t=mm(U[a0:b0,b0:b1],B[a0:b0,a0:b0],TN)
                B[b0:b1,a0:b0]=-mm(B[b0:b1,b0:b1],t,NN)
        size*=2
    S=jnp.concatenate([mm3(Gi[s*SUP:(s+1)*SUP,:(s+1)*SUP],y_ref[:(s+1)*SUP,:]) for s in range(sup)],0)
    v=jnp.sum(Li[...]*innov_ref[...],axis=1,keepdims=True)
    w=jnp.sum(Li[...]*v,axis=0,keepdims=True)
    hi=w.astype(BF).astype(F32)
    mid=(w-hi).astype(BF).astype(F32)
    pick=lax.broadcasted_iota(jnp.int32,w_ref.shape,0)
    w_ref[...]=jnp.where(pick==0,hi,jnp.where(pick==1,mid,jnp.where(pick==2,w-hi-mid,0.0))).astype(BF)
    for s in range(sup):
        z_ref[s*SUP:(s+1)*SUP,:]=mm(Li[s*SUP:,s*SUP:(s+1)*SUP],S[s*SUP:],TN).astype(z_ref.dtype)

def solve(y, innov, err):
    n,M=y.shape
    return pl.pallas_call(solve_kernel,
        out_shape=(jax.ShapeDtypeStruct((n,M),BF),jax.ShapeDtypeStruct((16,n),BF)),
        in_specs=[pl.BlockSpec(memory_space=pltpu.VMEM)]*4,
        out_specs=(pl.BlockSpec(memory_space=pltpu.VMEM),)*2,
        scratch_shapes=[pltpu.VMEM((n,n),F32)]*4,
        compiler_params=pltpu.CompilerParams(vmem_limit_bytes=40<<20),
        cost_estimate=pl.CostEstimate(flops=6*10**9,bytes_accessed=2<<20,transcendentals=0),
    )(y, innov[None,:], err[None,:], err[:,None])


def split3(x):
    hi = lax.reduce_precision(x, 8, 7)
    mid = lax.reduce_precision(x - hi, 8, 7)
    return hi, mid, x - hi - mid


def pack(anom, mean):
    cols = jnp.stack(split3(mean), axis=-1)
    cols = jnp.pad(cols, [(0, 0)] * (cols.ndim - 1) + [(0, 125)])
    return jnp.concatenate([anom, cols], axis=-1).astype(BF)


def unpack_sum(parts, members):
    total = jnp.sum(parts.astype(F32), axis=0)
    return total[..., :members], jnp.sum(total[..., members:], axis=-1)


def swap(array, axis):
    return lax.all_to_all(array, axis, split_axis=0, concat_axis=0, tiled=True)


def hits_of(codes, base, lanes):
    col = lax.broadcasted_iota(jnp.int32, (codes[0].shape[0], lanes), 1) + base
    total = jnp.where(codes[0] == col, 1.0, 0.0)
    for code in codes[1:]:
        total = total + jnp.where(code == col, 1.0, 0.0)
    return total.astype(BF)


def inner_kernel(code_ref, rows_ref, out_ref, same_ref, codes):
    step = pl.program_id(0)

    @pl.when(step == 0)
    def _():
        for k in range(codes.shape[0]):
            codes[k] = jnp.broadcast_to(code_ref[:, k : k + 1], codes.shape[1:])
        out_ref[...] = jnp.zeros_like(out_ref)

    wide = rows_ref.shape[0]
    parts = [codes[k] for k in range(codes.shape[0])]
    select = jnp.concatenate([hits_of(parts, step * wide + c, 128) for c in range(0, wide, 128)], axis=1)
    out_ref[...] += jnp.dot(select, rows_ref[...], preferred_element_type=F32)


def inner(code, rows):
    n_obs, slots = code.shape
    total, members = rows.shape
    wide = 256
    return pl.pallas_call(
        inner_kernel,
        out_shape=(
            jax.ShapeDtypeStruct((n_obs, members), F32),
            jax.ShapeDtypeStruct(rows.shape, rows.dtype),
        ),
        grid=(total // wide,),
        in_specs=[
            pl.BlockSpec((n_obs, slots), lambda i: (0, 0)),
            pl.BlockSpec((wide, members), lambda i: (i, 0)),
        ],
        out_specs=(
            pl.BlockSpec((n_obs, members), lambda i: (0, 0)),
            pl.BlockSpec(memory_space=pl.ANY),
        ),
        input_output_aliases={1: 1},
        scratch_shapes=[pltpu.VMEM((slots, n_obs, 128), jnp.int32)],
        cost_estimate=pl.CostEstimate(flops=2 * 10**9, bytes_accessed=2 << 20, transcendentals=0),
    )(code, rows)


def edge_kernel(first, code_ref, before_ref, after_ref, inner_ref, out_ref):
    n_obs, slots = code_ref.shape
    members = inner_ref.shape[1]
    wide = before_ref.shape[0]
    codes = [jnp.broadcast_to(code_ref[:, k : k + 1], (n_obs, wide)) for k in range(slots)]
    total = inner_ref[...]
    total += jnp.dot(hits_of(codes, first, wide), before_ref[...], preferred_element_type=F32)
    total += jnp.dot(hits_of(codes, first + wide, wide), after_ref[...], preferred_element_type=F32)
    total = total * (1.0 / KF)
    mean = jnp.sum(total, axis=1, keepdims=True) * (1.0 / members)
    out_ref[:, :members] = (total - mean).astype(BF)
    hi = mean.astype(BF).astype(F32)
    mid = (mean - hi).astype(BF).astype(F32)
    lane = lax.broadcasted_iota(jnp.int32, (n_obs, 128), 1)
    cols = jnp.where(lane == 0, hi, jnp.where(lane == 1, mid, jnp.where(lane == 2, mean - hi - mid, 0.0)))
    out_ref[:, members:] = cols.astype(BF)


def with_edges(first, code, before, after, part):
    n_obs, members = part.shape
    return pl.pallas_call(
        functools.partial(edge_kernel, first),
        out_shape=jax.ShapeDtypeStruct((n_obs, members + 128), BF),
        in_specs=[pl.BlockSpec(memory_space=pltpu.VMEM)] * 4,
        out_specs=pl.BlockSpec(memory_space=pltpu.VMEM),
        cost_estimate=pl.CostEstimate(flops=10**9, bytes_accessed=1 << 20, transcendentals=0),
    )(code, before, after, part)


def observe(grid, obs_col, obs_row, foot_off, obs_lev, ny_total):
    ny, nl, nx, members = grid.shape
    span = 2 * DY + 1
    x = obs_col[:, None] + foot_off // span - HW
    y = jnp.clip(obs_row[:, None] + foot_off % span - DY, 0, ny_total - 1) - lax.axis_index("gy") * ny
    lv = obs_lev[:, None] - lax.axis_index("lev") * nl
    inside = (y >= 0) & (y < ny) & (lv >= 0) & (lv < nl)
    place = y * nl + lv
    edge = ny * nl * HW
    total = ny * nl * nx
    low = total + place * HW + x + HW
    high = total + edge + place * HW + x - nx
    code = jnp.where(x < 0, low, jnp.where(x >= nx, high, place * nx + x))
    code = jnp.where(inside, code, -1)
    size = lax.axis_size("gx")
    up = [(i, (i + 1) % size) for i in range(size)]
    down = [(j, i) for i, j in up]
    before = lax.ppermute(grid[:, :, nx - HW :], "gx", up).reshape(edge, members)
    after = lax.ppermute(grid[:, :, :HW], "gx", down).reshape(edge, members)
    part, rows = inner(code, grid.reshape(total, members))
    return with_edges(total, code, before, after, part), rows


def share(msg):
    members = msg.shape[1] - 128
    for axis in ("lev", "gy"):
        size = lax.axis_size(axis)
        got = swap(msg.reshape(size, msg.shape[0] // size, msg.shape[1]), axis)
        msg = pack(*unpack_sum(got, members))
    size = lax.axis_size("gy")
    msg = swap(jnp.broadcast_to(msg[None], (size,) + msg.shape), "gy").reshape(-1, msg.shape[1])
    msg = lax.all_gather(msg, "lev", axis=0, tiled=True)
    return msg[:, :members], jnp.sum(msg[:, members : members + 3].astype(F32), axis=1)


def update_kernel(got_ref, loc_ref, y_ref, z_ref, w_ref, out_ref, mean_ref):
    nx = got_ref.shape[3]
    members = got_ref.shape[4]
    nl = got_ref.shape[2]
    levels = got_ref.shape[0] * nl
    rows = nx * levels
    ii = lax.broadcasted_iota(jnp.int32, (rows, rows), 0)
    jj = lax.broadcasted_iota(jnp.int32, (rows, rows), 1)
    order = jnp.where(jj == (ii % levels) * nx + ii // levels, 1.0, 0.0).astype(BF)
    for y in range(got_ref.shape[1]):
        block = jnp.concatenate([got_ref[lv // nl, y, lv % nl] for lv in range(levels)], axis=0)
        block = jnp.dot(order, block, preferred_element_type=F32)
        xbar = jnp.sum(block, axis=1, keepdims=True) * (1.0 / members)
        anom = (block - xbar).astype(BF)
        cross = mm(anom, y_ref[...], NT, None) * (1.0 / (members - 1))
        weight = loc_ref[y].astype(F32)
        weight = jnp.broadcast_to(weight[:, None, :], (nx, levels, weight.shape[1])).reshape(rows, weight.shape[1])
        gain = (cross * weight).astype(BF)
        result = anom.astype(F32) - jnp.dot(gain, z_ref[...], preferred_element_type=F32)
        out_ref[:, y] = result.reshape(nx, levels, members).astype(BF)
        shift = jnp.sum(mm(gain, w_ref[...], NT, None), axis=1, keepdims=True)
        mean = jnp.where(ii == jj, xbar + shift, 0.0)
        mean_ref[0, y : y + 1] = jnp.sum(mean, axis=0, keepdims=True)


def update(got, loc, ybf, zmat, wrows):
    parts, ny, nl, nx, members = got.shape
    n_obs = ybf.shape[0]
    levels = parts * nl
    wide = 16
    whole = lambda i: (0, 0)
    out, mean = pl.pallas_call(
        update_kernel,
        out_shape=(
            jax.ShapeDtypeStruct((nx, ny, levels, members), BF),
            jax.ShapeDtypeStruct((nx // wide, ny, wide * levels), F32),
        ),
        grid=(nx // wide,),
        in_specs=[
            pl.BlockSpec((parts, ny, nl, wide, members), lambda i: (0, 0, 0, i, 0)),
            pl.BlockSpec((ny, wide, n_obs), lambda i: (0, i, 0)),
            pl.BlockSpec(ybf.shape, whole),
            pl.BlockSpec(zmat.shape, whole),
            pl.BlockSpec(wrows.shape, whole),
        ],
        out_specs=(
            pl.BlockSpec((wide, ny, levels, members), lambda i: (i, 0, 0, 0)),
            pl.BlockSpec((1, ny, wide * levels), lambda i: (i, 0, 0)),
        ),
        cost_estimate=pl.CostEstimate(flops=3 * 10**9, bytes_accessed=5 << 20, transcendentals=0),
    )(got, loc, ybf, zmat, wrows)
    mean = mean.reshape(nx // wide, ny, wide, levels).transpose(0, 2, 1, 3).reshape(nx, ny, levels)
    return mean, out


def local(state, obs_col, obs_row, foot_off, obs_lev, obs_val, obs_err, loc):
    nx, ny, nl, members = state.shape
    grid = lax.optimization_barrier(jnp.transpose(state, (1, 2, 0, 3)))
    msg, grid = observe(grid, obs_col, obs_row, foot_off, obs_lev, ny * lax.axis_size("gy"))
    ybf, hbar = share(msg)
    size = lax.axis_size("lev")
    grid, ybf, hbar = lax.optimization_barrier((grid, ybf, hbar))
    got = swap(grid.reshape(size, ny // size, nl, nx, members), "lev")
    zmat, wrows = solve(ybf, obs_val - hbar, obs_err)
    return update(got, jnp.transpose(loc, (1, 0, 2)), ybf, zmat, wrows)


def solution(mesh):
    return jax.shard_map(
        local,
        mesh=mesh,
        in_specs=(
            P("gx", "gy", "lev", None),
            P("gx"),
            P("gx"),
            P("gx", None),
            P("gx"),
            P("gx"),
            P("gx"),
            P("gx", ("gy", "lev"), None),
        ),
        out_specs=(P("gx", ("gy", "lev"), None), P("gx", ("gy", "lev"), None, None)),
        check_vma=False,
    )
```

```python
import functools

import jax, jax.numpy as jnp
from jax import lax
from jax.experimental import pallas as pl
from jax.experimental.pallas import tpu as pltpu
from jax.sharding import PartitionSpec as P

KF = 8
HW = 8
DY = 2
F32=jnp.float32
BF=jnp.bfloat16
HI=lax.Precision.HIGHEST
SUB=32
SUP=128

def mm(a,b,dims,prec=HI):
    return lax.dot_general(a,b,(dims,((),())),precision=prec,preferred_element_type=F32)
def halves(a):
    hi=a.astype(BF)
    return hi,(a-hi.astype(F32)).astype(BF)
NN=((1,),(0,)); NT=((1,),(1,)); TN=((0,),(0,))

def factor_block(R, off, sq):
    nv=SUB//8
    row=lax.broadcasted_iota(jnp.int32,(8,128),0)
    lane=lax.broadcasted_iota(jnp.int32,(8,128),1)
    C=[[jnp.broadcast_to(R[8*v:8*v+8, off+j:off+j+1],(8,128)) if v>=j//8 else None for v in range(nv)] for j in range(SUB)]
    X=[jnp.where(lane==row+8*v,1.0,0.0).astype(F32) for v in range(nv)]
    G=list(X)
    rs=[jnp.zeros((8,128),F32) for _ in range(nv)]
    def rowb(t,i):
        return jnp.broadcast_to(t[i:i+1,:],(8,128))
    for j in range(SUB):
        vj,ij=divmod(j,8)
        p=rowb(C[j][vj],ij)
        inv=1.0/p
        col=[C[j][v] if v>=vj else None for v in range(nv)]
        q=[None if c is None else c*inv for c in col]
        for k in range(j+1,SUB):
            vk,ik=divmod(k,8)
            ck=rowb(col[vk],ik)
            for v in range(vk,nv):
                C[k][v]=C[k][v]-q[v]*ck
        r=lax.rsqrt(p)
        below=row>ij
        qm=[None if t is None else t for t in q]
        qm[vj]=jnp.where(below,q[vj],0.0)
        rs[vj]=jnp.where(row==ij,r,rs[vj])
        sp=p*r
        xj=rowb(X[vj],ij)
        g=1.0/(sp+rowb(sq[vj],ij))
        gj=rowb(G[vj],ij)*g
        G[vj]=jnp.where(row==ij,gj,G[vj])
        gs=gj*sp
        for v in range(vj,nv):
            X[v]=X[v]-qm[v]*xj
            G[v]=G[v]-qm[v]*gs
    X=[X[v]*rs[v] for v in range(nv)]
    return jnp.concatenate(X,0)[:,:SUB], jnp.concatenate(G,0)[:,:SUB]

def solve_kernel(y_ref, innov_ref, errr_ref, errc_ref, z_ref, w_ref, A, U, Li, Gi):
    n=A.shape[0]
    M=y_ref.shape[1]
    y=y_ref[...]
    A[...]=mm(y,y,NT,None)*(1.0/(M-1))
    Li[...]=jnp.zeros_like(Li)
    Gi[...]=jnp.zeros_like(Gi)
    sup=n//SUP
    ii=lax.broadcasted_iota(jnp.int32,(SUP,SUP),0)
    jj=lax.broadcasted_iota(jnp.int32,(SUP,SUP),1)
    for s in range(sup):
        w0=s*SUP
        A[w0:w0+SUP,w0:w0+SUP]=A[w0:w0+SUP,w0:w0+SUP]+jnp.where(ii==jj,errr_ref[:,w0:w0+SUP],0.0)
    for s in range(sup):
        w0=s*SUP
        for t in range(SUP//SUB):
            k0=w0+t*SUB
            R=A[k0:k0+SUB,w0:n]
            if t:
                R=R-mm(U[w0:k0,k0:k0+SUB],U[w0:k0,w0:n],TN)
            sq=jnp.broadcast_to(jnp.sqrt(errc_ref[k0:k0+SUB,:]),(SUB,128))
            sq=[sq[8*v:8*v+8] for v in range(SUB//8)]
            x,g=factor_block(R,t*SUB,sq)
            U[k0:k0+SUB,w0:n]=mm(x,R,NN)
            Li[k0:k0+SUB,k0:k0+SUB]=x
            Gi[k0:k0+SUB,k0:k0+SUB]=g
        w1=w0+SUP
        if w1<n:
            A[w1:n,w1:n]=A[w1:n,w1:n]-mm(U[w0:w1,w1:n],U[w0:w1,w1:n],TN)
    for s in range(sup):
        w0=s*SUP
        L=U[w0:w0+SUP,w0:w0+SUP].T
        for B in (Li,Gi):
            T=B[w0:w0+SUP,w0:w0+SUP]
            size=SUB
            while size<SUP:
                mask=((ii//(2*size))==(jj//(2*size)))&((ii//size)>(jj//size))
                N=jnp.where(mask,L,0.0)
                T=T-mm(T,mm(N,T,NN),NN)
                size*=2
            B[w0:w0+SUP,w0:w0+SUP]=T
    size=SUP
    while size<n:
        for a0 in range(0,n,2*size):
            b0=a0+size; b1=b0+size
            for B in (Li,Gi):
                t=mm(U[a0:b0,b0:b1],B[a0:b0,a0:b0],TN)
                B[b0:b1,a0:b0]=-mm(B[b0:b1,b0:b1],t,NN)
        size*=2
    gh,gl=halves(Gi[...])
    S=[]
    for s in range(sup):
        r,k=slice(s*SUP,(s+1)*SUP),(s+1)*SUP
        S.append(mm(gh[r,:k],y[:k],NN,None)+mm(gl[r,:k],y[:k],NN,None))
    sh,sl=halves(jnp.concatenate(S,0))
    lh,ll=halves(Li[...].T)
    v=jnp.sum(Li[...]*innov_ref[...],axis=1,keepdims=True)
    w=jnp.sum(Li[...]*v,axis=0,keepdims=True)
    hi=w.astype(BF).astype(F32)
    mid=(w-hi).astype(BF).astype(F32)
    pick=lax.broadcasted_iota(jnp.int32,w_ref.shape,0)
    w_ref[...]=jnp.where(pick==0,hi,jnp.where(pick==1,mid,jnp.where(pick==2,w-hi-mid,0.0))).astype(BF)
    for s in range(sup):
        r,k=slice(s*SUP,(s+1)*SUP),s*SUP
        z=mm(lh[r,k:],sh[k:],NN,None)+(mm(lh[r,k:],sl[k:],NN,None)+mm(ll[r,k:],sh[k:],NN,None))
        z_ref[r,:]=z.astype(z_ref.dtype)

def solve(y, innov, err):
    n,M=y.shape
    return pl.pallas_call(solve_kernel,
        out_shape=(jax.ShapeDtypeStruct((n,M),BF),jax.ShapeDtypeStruct((16,n),BF)),
        in_specs=[pl.BlockSpec(memory_space=pltpu.VMEM)]*4,
        out_specs=(pl.BlockSpec(memory_space=pltpu.VMEM),)*2,
        scratch_shapes=[pltpu.VMEM((n,n),F32)]*4,
        compiler_params=pltpu.CompilerParams(vmem_limit_bytes=24<<20),
        cost_estimate=pl.CostEstimate(flops=6*10**9,bytes_accessed=2<<20,transcendentals=0),
    )(y, innov[None,:], err[None,:], err[:,None])


def split3(x):
    hi = lax.reduce_precision(x, 8, 7)
    mid = lax.reduce_precision(x - hi, 8, 7)
    return hi, mid, x - hi - mid


def pack(anom, mean):
    cols = jnp.stack(split3(mean), axis=-1)
    cols = jnp.pad(cols, [(0, 0)] * (cols.ndim - 1) + [(0, 125)])
    return jnp.concatenate([anom, cols], axis=-1).astype(BF)


def unpack_sum(parts, members):
    total = jnp.sum(parts.astype(F32), axis=0)
    return total[..., :members], jnp.sum(total[..., members:], axis=-1)


def swap(array, axis):
    return lax.all_to_all(array, axis, split_axis=0, concat_axis=0, tiled=True)


def hits_of(codes, base, lanes):
    col = lax.broadcasted_iota(jnp.int32, (codes[0].shape[0], lanes), 1) + base
    total = jnp.where(codes[0] == col, 1.0, 0.0)
    for code in codes[1:]:
        total = total + jnp.where(code == col, 1.0, 0.0)
    return total.astype(BF)


def codes_of(ny_total, ny, nl, nx, col_ref, row_ref, lev_ref, foot_ref):
    foot = foot_ref[...]
    shift_x = lax.shift_right_logical(foot * 205, 10)
    shift_y = foot - (2 * DY + 1) * shift_x
    x = col_ref[...] + shift_x - HW
    y = jnp.clip(row_ref[...] + shift_y - DY, 0, ny_total - 1) - lax.axis_index("gy") * ny
    lv = lev_ref[...] - lax.axis_index("lev") * nl
    inside = (y >= 0) & (y < ny) & (lv >= 0) & (lv < nl)
    place = y * nl + lv
    edge = ny * nl * HW
    total = ny * nl * nx
    low = total + place * HW + x + HW
    high = total + edge + place * HW + x - nx
    code = jnp.where(x < 0, low, jnp.where(x >= nx, high, place * nx + x))
    return jnp.where(inside, code, -1).T


def inner_kernel(dims, wide, col_ref, row_ref, lev_ref, foot_ref, rows_ref, out_ref, same_ref, codes):
    step = pl.program_id(0)

    @pl.when(step == 0)
    def _():
        code = codes_of(*dims, col_ref, row_ref, lev_ref, foot_ref)
        for k in range(codes.shape[0]):
            codes[k] = jnp.broadcast_to(code[:, k : k + 1], codes.shape[1:])

    parts = [codes[k] for k in range(codes.shape[0])]
    select = jnp.concatenate([hits_of(parts, step * wide + c, 128) for c in range(0, wide, 128)], axis=1)
    rows = rows_ref[pl.ds(pl.multiple_of(step * wide, wide), wide), :]
    part = jnp.dot(select, rows, preferred_element_type=F32)

    @pl.when(step == 0)
    def _():
        out_ref[...] = part

    @pl.when(step > 0)
    def _():
        out_ref[...] += part


VM = pl.BlockSpec(memory_space=pltpu.VMEM)


def inner(dims, index, rows):
    slots, n_obs = index[3].shape
    total, members = rows.shape
    wide = 512
    return pl.pallas_call(
        functools.partial(inner_kernel, dims, wide),
        out_shape=(
            jax.ShapeDtypeStruct((n_obs, members), F32),
            jax.ShapeDtypeStruct(rows.shape, rows.dtype),
        ),
        grid=(total // wide,),
        in_specs=[VM] * 5,
        out_specs=(VM, pl.BlockSpec(memory_space=pl.ANY)),
        input_output_aliases={4: 1},
        scratch_shapes=[pltpu.VMEM((slots, n_obs, 128), jnp.int32)],
        compiler_params=pltpu.CompilerParams(vmem_limit_bytes=24 << 20),
        cost_estimate=pl.CostEstimate(flops=2 * 10**9, bytes_accessed=2 << 20, transcendentals=0),
    )(*index, rows)


def edge_kernel(dims, col_ref, row_ref, lev_ref, foot_ref, before_ref, after_ref, inner_ref, out_ref):
    n_obs, members = inner_ref.shape
    wide = before_ref.shape[0]
    first = dims[1] * dims[2] * dims[3]
    code = codes_of(*dims, col_ref, row_ref, lev_ref, foot_ref)
    codes = [jnp.broadcast_to(code[:, k : k + 1], (n_obs, wide)) for k in range(code.shape[1])]
    select = jnp.concatenate([hits_of(codes, first, wide), hits_of(codes, first + wide, wide)], axis=1)
    rows = jnp.concatenate([before_ref[...], after_ref[...]], axis=0)
    total = inner_ref[...] + jnp.dot(select, rows, preferred_element_type=F32)
    total = total * (1.0 / KF)
    mean = jnp.sum(total, axis=1, keepdims=True) * (1.0 / members)
    out_ref[:, :members] = (total - mean).astype(BF)
    hi = mean.astype(BF).astype(F32)
    mid = (mean - hi).astype(BF).astype(F32)
    lane = lax.broadcasted_iota(jnp.int32, (n_obs, 128), 1)
    cols = jnp.where(lane == 0, hi, jnp.where(lane == 1, mid, jnp.where(lane == 2, mean - hi - mid, 0.0)))
    out_ref[:, members:] = cols.astype(BF)


def with_edges(dims, index, before, after, part):
    n_obs, members = part.shape
    return pl.pallas_call(
        functools.partial(edge_kernel, dims),
        out_shape=jax.ShapeDtypeStruct((n_obs, members + 128), BF),
        in_specs=[VM] * 7,
        out_specs=VM,
        compiler_params=pltpu.CompilerParams(vmem_limit_bytes=24 << 20),
        cost_estimate=pl.CostEstimate(flops=10**9, bytes_accessed=1 << 20, transcendentals=0),
    )(*index, before, after, part)


def observe(grid, obs_col, obs_row, foot_off, obs_lev, ny_total):
    ny, nl, nx, members = grid.shape
    dims = (ny_total, ny, nl, nx)
    index = (obs_col[None, :], obs_row[None, :], obs_lev[None, :], foot_off.T)
    size = lax.axis_size("gx")
    up = [(i, (i + 1) % size) for i in range(size)]
    down = [(j, i) for i, j in up]
    edge = ny * nl * HW
    before = lax.ppermute(grid[:, :, nx - HW :], "gx", up).reshape(edge, members)
    after = lax.ppermute(grid[:, :, :HW], "gx", down).reshape(edge, members)
    part, rows = inner(dims, index, grid.reshape(ny * nl * nx, members))
    return with_edges(dims, index, before, after, part), rows


def share(msg):
    members = msg.shape[1] - 128
    for axis in ("lev", "gy"):
        size = lax.axis_size(axis)
        got = swap(msg.reshape(size, msg.shape[0] // size, msg.shape[1]), axis)
        msg = pack(*unpack_sum(got, members))
    for axis in ("gy", "lev"):
        size = lax.axis_size(axis)
        msg = swap(jnp.broadcast_to(msg[None], (size,) + msg.shape), axis).reshape(-1, msg.shape[1])
    return msg[:, :members], jnp.sum(msg[:, members : members + 3].astype(F32), axis=1)


def update_kernel(got_ref, loc_ref, y_ref, z_ref, w_ref, out_ref, mean_ref):
    parts, ny, nl, nx, members = got_ref.shape
    levels = parts * nl
    part = 16
    rows = part * levels
    step = pl.program_id(0)
    ii = lax.broadcasted_iota(jnp.int32, (rows, rows), 0)
    jj = lax.broadcasted_iota(jnp.int32, (rows, rows), 1)
    order = jnp.where(jj == (ii % levels) * part + ii // levels, 1.0, 0.0).astype(BF)
    blocks, weights = [], []
    for y in range(ny):
        for x in range(0, nx, part):
            block = jnp.concatenate(
                [got_ref[lv // nl, y, lv % nl, x : x + part] for lv in range(levels)], axis=0
            )
            blocks.append(jnp.dot(order, block, preferred_element_type=F32))
        weight = loc_ref[y].astype(F32)
        weight = jnp.broadcast_to(weight[:, None, :], (nx, levels, weight.shape[1]))
        weights.append(weight.reshape(nx * levels, weight.shape[2]))
    block = jnp.concatenate(blocks, axis=0)
    xbar = jnp.sum(block, axis=1, keepdims=True) * (1.0 / members)
    anom = (block - xbar).astype(BF)
    cross = mm(anom, y_ref[...], NT, None) * (1.0 / (members - 1))
    gain = (cross * jnp.concatenate(weights, axis=0)).astype(BF)
    result = anom.astype(F32) - jnp.dot(gain, z_ref[...], preferred_element_type=F32)
    result = result.reshape(ny, nx, levels, members).astype(BF)
    column = xbar + jnp.sum(mm(gain, w_ref[...], NT, None), axis=1, keepdims=True)
    count = nx * levels
    lane = lax.broadcasted_iota(jnp.int32, (count, 128), 1)
    place = lax.broadcasted_iota(jnp.int32, (count, 128), 0) // levels + step * nx

    @pl.when(step == 0)
    def _():
        mean_ref[...] = jnp.zeros_like(mean_ref)

    for y in range(ny):
        out_ref[:, y] = result[y]
        spread = jnp.where(lane == place, column[y * count : (y + 1) * count], 0.0)
        mean_ref[y] += jnp.sum(spread.reshape(nx, levels, 128), axis=0)


def update(got, loc, ybf, zmat, wrows):
    parts, ny, nl, nx, members = got.shape
    n_obs = ybf.shape[0]
    levels = parts * nl
    wide = 32
    out, mean = pl.pallas_call(
        update_kernel,
        out_shape=(
            jax.ShapeDtypeStruct((nx, ny, levels, members), BF),
            jax.ShapeDtypeStruct((ny, levels, nx), F32),
        ),
        grid=(nx // wide,),
        in_specs=[
            pl.BlockSpec((parts, ny, nl, wide, members), lambda i: (0, 0, 0, i, 0)),
            pl.BlockSpec((ny, wide, n_obs), lambda i: (0, i, 0)),
            VM,
            VM,
            VM,
        ],
        out_specs=(
            pl.BlockSpec((wide, ny, levels, members), lambda i: (i, 0, 0, 0)),
            pl.BlockSpec((ny, levels, nx), lambda i: (0, 0, 0)),
        ),
        compiler_params=pltpu.CompilerParams(vmem_limit_bytes=24 << 20),
        cost_estimate=pl.CostEstimate(flops=3 * 10**9, bytes_accessed=5 << 20, transcendentals=0),
    )(got, loc, ybf, zmat, wrows)
    return mean.transpose(2, 0, 1), out


def local(state, obs_col, obs_row, foot_off, obs_lev, obs_val, obs_err, loc):
    nx, ny, nl, members = state.shape
    grid = lax.optimization_barrier(jnp.transpose(state, (1, 2, 0, 3)))
    msg, grid = observe(grid, obs_col, obs_row, foot_off, obs_lev, ny * lax.axis_size("gy"))
    ybf, hbar = share(msg)
    size = lax.axis_size("lev")
    grid, ybf, hbar = lax.optimization_barrier((grid, ybf, hbar))
    got = swap(grid.reshape(size, ny // size, nl, nx, members), "lev")
    zmat, wrows = solve(ybf, obs_val - hbar, obs_err)
    return update(got, jnp.transpose(loc, (1, 0, 2)), ybf, zmat, wrows)


def solution(mesh):
    return jax.shard_map(
        local,
        mesh=mesh,
        in_specs=(
            P("gx", "gy", "lev", None),
            P("gx"),
            P("gx"),
            P("gx", None),
            P("gx"),
            P("gx"),
            P("gx"),
            P("gx", ("gy", "lev"), None),
        ),
        out_specs=(P("gx", ("gy", "lev"), None), P("gx", ("gy", "lev"), None, None)),
        check_vma=False,
    )
```

```python
import functools

import jax, jax.numpy as jnp
from jax import lax
from jax.experimental import pallas as pl
from jax.experimental.pallas import tpu as pltpu
from jax.sharding import PartitionSpec as P

KF = 8
HW = 8
DY = 2
F32=jnp.float32
BF=jnp.bfloat16
HI=lax.Precision.HIGHEST
SUB=32
SUP=128

def mm(a,b,dims,prec=HI):
    return lax.dot_general(a,b,(dims,((),())),precision=prec,preferred_element_type=F32)
def halves(a):
    hi=a.astype(BF)
    return hi,(a-hi.astype(F32)).astype(BF)
NN=((1,),(0,)); NT=((1,),(1,)); TN=((0,),(0,))

def factor_block(R, off, sq):
    nv=SUB//8
    row=lax.broadcasted_iota(jnp.int32,(8,128),0)
    lane=lax.broadcasted_iota(jnp.int32,(8,128),1)
    C=[[jnp.broadcast_to(R[8*v:8*v+8, off+j:off+j+1],(8,128)) if v>=j//8 else None for v in range(nv)] for j in range(SUB)]
    X=[jnp.where(lane==row+8*v,1.0,0.0).astype(F32) for v in range(nv)]
    G=list(X)
    rs=[jnp.zeros((8,128),F32) for _ in range(nv)]
    def rowb(t,i):
        return jnp.broadcast_to(t[i:i+1,:],(8,128))
    for j in range(SUB):
        vj,ij=divmod(j,8)
        p=rowb(C[j][vj],ij)
        inv=1.0/p
        col=[C[j][v] if v>=vj else None for v in range(nv)]
        q=[None if c is None else c*inv for c in col]
        for k in range(j+1,SUB):
            vk,ik=divmod(k,8)
            ck=rowb(col[vk],ik)
            for v in range(vk,nv):
                C[k][v]=C[k][v]-q[v]*ck
        r=lax.rsqrt(p)
        below=row>ij
        qm=[None if t is None else t for t in q]
        qm[vj]=jnp.where(below,q[vj],0.0)
        rs[vj]=jnp.where(row==ij,r,rs[vj])
        sp=p*r
        xj=rowb(X[vj],ij)
        g=1.0/(sp+rowb(sq[vj],ij))
        gj=rowb(G[vj],ij)*g
        G[vj]=jnp.where(row==ij,gj,G[vj])
        gs=gj*sp
        for v in range(vj,nv):
            X[v]=X[v]-qm[v]*xj
            G[v]=G[v]-qm[v]*gs
    X=[X[v]*rs[v] for v in range(nv)]
    return jnp.concatenate(X,0)[:,:SUB], jnp.concatenate(G,0)[:,:SUB]

def mm_split(a,b,dims):
    ah,al=halves(a)
    bh,bl=halves(b)
    return mm(ah,bh,dims,None)+(mm(ah,bl,dims,None)+mm(al,bh,dims,None))

def solve_kernel(y_ref, innov_ref, errr_ref, errc_ref, z_ref, w_ref, A, U, Li, Gi, S, V):
    n=A.shape[0]
    M=y_ref.shape[1]
    y=y_ref[...]
    A[...]=mm(y,y,NT,None)*(1.0/(M-1))
    sup=n//SUP
    ii=lax.broadcasted_iota(jnp.int32,(SUP,SUP),0)
    jj=lax.broadcasted_iota(jnp.int32,(SUP,SUP),1)
    for s in range(sup):
        w0=s*SUP
        A[w0:w0+SUP,w0:w0+SUP]=A[w0:w0+SUP,w0:w0+SUP]+jnp.where(ii==jj,errr_ref[:,w0:w0+SUP],0.0)
    Li[...]=jnp.zeros_like(Li)
    Gi[...]=jnp.zeros_like(Gi)

    def lower(w0,q):
        def run():
            r=slice(q,q+SUP)
            A[r,q:n]=A[r,q:n]-mm(U[w0:w0+SUP,r],U[w0:w0+SUP,q:n],TN)
        return run

    def widen(B,w0,size):
        def run():
            L=U[w0:w0+SUP,w0:w0+SUP].T
            T=B[w0:w0+SUP,:]
            mask=((ii//(2*size))==(jj//(2*size)))&((ii//size)>(jj//size))
            B[w0:w0+SUP,:]=T-mm(T,mm(jnp.where(mask,L,0.0),T,NN),NN)
        return run

    def ahead_s(w0):
        def run():
            r=slice(w0,w0+SUP)
            rest=y_ref[r,:].astype(F32)
            if w0:
                rest=rest-mm_split(U[:w0,r],S[:w0,:],TN)
            S[r,:]=mm_split(Gi[r,:],rest,NN)
        return run

    def ahead_v(w0):
        def run():
            r=slice(w0,w0+SUP)
            rest=jnp.broadcast_to(innov_ref[r,:],(SUP,128))
            if w0:
                rest=rest-mm(U[:w0,r],V[:w0,:],TN)
            V[r,:]=mm(Li[r,:],rest,NN)
        return run

    waiting=[]
    for s in range(sup):
        w0=s*SUP
        for t in range(SUP//SUB):
            k0=w0+t*SUB
            R=A[k0:k0+SUB,w0:n]
            if t:
                R=R-mm(U[w0:k0,k0:k0+SUB],U[w0:k0,w0:n],TN)
            for task in waiting[:2]:
                task()
            waiting=waiting[2:]
            sq=jnp.broadcast_to(jnp.sqrt(errc_ref[k0:k0+SUB,:]),(SUB,128))
            sq=[sq[8*v:8*v+8] for v in range(SUB//8)]
            x,g=factor_block(R,t*SUB,sq)
            U[k0:k0+SUB,w0:n]=mm(x,R,NN)
            Li[k0:k0+SUB,t*SUB:(t+1)*SUB]=x
            Gi[k0:k0+SUB,t*SUB:(t+1)*SUB]=g
        w1=w0+SUP
        if w1<n:
            lower(w0,w1)()
        for task in waiting:
            task()
        waiting=[lower(w0,q) for q in range(w1+SUP,n,SUP)]
        waiting+=[widen(Gi,w0,SUB),widen(Li,w0,SUB),widen(Gi,w0,2*SUB),widen(Li,w0,2*SUB),ahead_s(w0),ahead_v(w0)]
    for task in waiting:
        task()
    for s in reversed(range(sup)):
        r=slice(s*SUP,(s+1)*SUP)
        k=(s+1)*SUP
        lt=Li[r,:].T
        rest,tail=S[r,:],V[r,:]
        if k<n:
            rest=rest-mm_split(U[r,k:],S[k:,:],NN)
            tail=tail-mm(U[r,k:],V[k:,:],NN)
        z=mm_split(lt,rest,NN)
        S[r,:]=z
        z_ref[r,:]=z.astype(z_ref.dtype)
        V[r,:]=mm(lt,tail,NN)
    w=V[...].T[0:1,:]
    hi=w.astype(BF).astype(F32)
    mid=(w-hi).astype(BF).astype(F32)
    pick=lax.broadcasted_iota(jnp.int32,w_ref.shape,0)
    w_ref[...]=jnp.where(pick==0,hi,jnp.where(pick==1,mid,jnp.where(pick==2,w-hi-mid,0.0))).astype(BF)

def solve(y, innov, err):
    n,M=y.shape
    return pl.pallas_call(solve_kernel,
        out_shape=(jax.ShapeDtypeStruct((n,M),BF),jax.ShapeDtypeStruct((16,n),BF)),
        in_specs=[pl.BlockSpec(memory_space=pltpu.VMEM)]*4,
        out_specs=(pl.BlockSpec(memory_space=pltpu.VMEM),)*2,
        scratch_shapes=[pltpu.VMEM((n,n),F32)]*2+[pltpu.VMEM((n,SUP),F32)]*2+[pltpu.VMEM((n,M),F32),pltpu.VMEM((n,128),F32)],
        compiler_params=pltpu.CompilerParams(vmem_limit_bytes=24<<20),
        cost_estimate=pl.CostEstimate(flops=6*10**9,bytes_accessed=2<<20,transcendentals=0),
    )(y, innov[:,None], err[None,:], err[:,None])


def split3(x):
    hi = lax.reduce_precision(x, 8, 7)
    mid = lax.reduce_precision(x - hi, 8, 7)
    return hi, mid, x - hi - mid


def pack(anom, mean):
    cols = jnp.stack(split3(mean), axis=-1)
    cols = jnp.pad(cols, [(0, 0)] * (cols.ndim - 1) + [(0, 125)])
    return jnp.concatenate([anom, cols], axis=-1).astype(BF)


def unpack_sum(parts, members):
    total = jnp.sum(parts.astype(F32), axis=0)
    return total[..., :members], jnp.sum(total[..., members:], axis=-1)


def swap(array, axis):
    return lax.all_to_all(array, axis, split_axis=0, concat_axis=0, tiled=True)


def hits_of(codes, base, lanes):
    col = lax.broadcasted_iota(jnp.int32, (codes[0].shape[0], lanes), 1) + base
    total = jnp.where(codes[0] == col, 1.0, 0.0)
    for code in codes[1:]:
        total = total + jnp.where(code == col, 1.0, 0.0)
    return total.astype(BF)


def codes_of(ny_total, ny, nl, nx, col_ref, row_ref, lev_ref, foot_ref):
    foot = foot_ref[...]
    shift_x = lax.shift_right_logical(foot * 205, 10)
    shift_y = foot - (2 * DY + 1) * shift_x
    x = col_ref[...] + shift_x - HW
    y = jnp.clip(row_ref[...] + shift_y - DY, 0, ny_total - 1) - lax.axis_index("gy") * ny
    lv = lev_ref[...] - lax.axis_index("lev") * nl
    inside = (y >= 0) & (y < ny) & (lv >= 0) & (lv < nl)
    place = y * nl + lv
    edge = ny * nl * HW
    total = ny * nl * nx
    low = total + place * HW + x + HW
    high = total + edge + place * HW + x - nx
    code = jnp.where(x < 0, low, jnp.where(x >= nx, high, place * nx + x))
    return jnp.where(inside, code, -1).T


def inner_kernel(dims, wide, col_ref, row_ref, lev_ref, foot_ref, rows_ref, out_ref, same_ref, codes):
    step = pl.program_id(0)

    @pl.when(step == 0)
    def _():
        code = codes_of(*dims, col_ref, row_ref, lev_ref, foot_ref)
        for k in range(codes.shape[0]):
            codes[k] = jnp.broadcast_to(code[:, k : k + 1], codes.shape[1:])

    parts = [codes[k] for k in range(codes.shape[0])]
    select = jnp.concatenate([hits_of(parts, step * wide + c, 128) for c in range(0, wide, 128)], axis=1)
    rows = rows_ref[pl.ds(pl.multiple_of(step * wide, wide), wide), :]
    part = jnp.dot(select, rows, preferred_element_type=F32)

    @pl.when(step == 0)
    def _():
        out_ref[...] = part

    @pl.when(step > 0)
    def _():
        out_ref[...] += part


VM = pl.BlockSpec(memory_space=pltpu.VMEM)


def inner(dims, index, rows):
    slots, n_obs = index[3].shape
    total, members = rows.shape
    wide = 512
    return pl.pallas_call(
        functools.partial(inner_kernel, dims, wide),
        out_shape=(
            jax.ShapeDtypeStruct((n_obs, members), F32),
            jax.ShapeDtypeStruct(rows.shape, rows.dtype),
        ),
        grid=(total // wide,),
        in_specs=[VM] * 5,
        out_specs=(VM, pl.BlockSpec(memory_space=pl.ANY)),
        input_output_aliases={4: 1},
        scratch_shapes=[pltpu.VMEM((slots, n_obs, 128), jnp.int32)],
        compiler_params=pltpu.CompilerParams(vmem_limit_bytes=24 << 20),
        cost_estimate=pl.CostEstimate(flops=2 * 10**9, bytes_accessed=2 << 20, transcendentals=0),
    )(*index, rows)


def edge_kernel(dims, col_ref, row_ref, lev_ref, foot_ref, before_ref, after_ref, inner_ref, out_ref):
    n_obs, members = inner_ref.shape
    wide = before_ref.shape[0]
    first = dims[1] * dims[2] * dims[3]
    code = codes_of(*dims, col_ref, row_ref, lev_ref, foot_ref)
    codes = [jnp.broadcast_to(code[:, k : k + 1], (n_obs, wide)) for k in range(code.shape[1])]
    select = jnp.concatenate([hits_of(codes, first, wide), hits_of(codes, first + wide, wide)], axis=1)
    rows = jnp.concatenate([before_ref[...], after_ref[...]], axis=0)
    total = inner_ref[...] + jnp.dot(select, rows, preferred_element_type=F32)
    total = total * (1.0 / KF)
    mean = jnp.sum(total, axis=1, keepdims=True) * (1.0 / members)
    out_ref[:, :members] = (total - mean).astype(BF)
    hi = mean.astype(BF).astype(F32)
    mid = (mean - hi).astype(BF).astype(F32)
    lane = lax.broadcasted_iota(jnp.int32, (n_obs, 128), 1)
    cols = jnp.where(lane == 0, hi, jnp.where(lane == 1, mid, jnp.where(lane == 2, mean - hi - mid, 0.0)))
    out_ref[:, members:] = cols.astype(BF)


def with_edges(dims, index, before, after, part):
    n_obs, members = part.shape
    return pl.pallas_call(
        functools.partial(edge_kernel, dims),
        out_shape=jax.ShapeDtypeStruct((n_obs, members + 128), BF),
        in_specs=[VM] * 7,
        out_specs=VM,
        compiler_params=pltpu.CompilerParams(vmem_limit_bytes=24 << 20),
        cost_estimate=pl.CostEstimate(flops=10**9, bytes_accessed=1 << 20, transcendentals=0),
    )(*index, before, after, part)


def observe(grid, obs_col, obs_row, foot_off, obs_lev, ny_total):
    ny, nl, nx, members = grid.shape
    dims = (ny_total, ny, nl, nx)
    index = (obs_col[None, :], obs_row[None, :], obs_lev[None, :], foot_off.T)
    size = lax.axis_size("gx")
    up = [(i, (i + 1) % size) for i in range(size)]
    down = [(j, i) for i, j in up]
    edge = ny * nl * HW
    before = lax.ppermute(grid[:, :, nx - HW :], "gx", up).reshape(edge, members)
    after = lax.ppermute(grid[:, :, :HW], "gx", down).reshape(edge, members)
    part, rows = inner(dims, index, grid.reshape(ny * nl * nx, members))
    return with_edges(dims, index, before, after, part), rows


def share(msg):
    members = msg.shape[1] - 128
    for axis in ("lev", "gy"):
        size = lax.axis_size(axis)
        got = swap(msg.reshape(size, msg.shape[0] // size, msg.shape[1]), axis)
        msg = pack(*unpack_sum(got, members))
    for axis in ("gy", "lev"):
        size = lax.axis_size(axis)
        msg = swap(jnp.broadcast_to(msg[None], (size,) + msg.shape), axis).reshape(-1, msg.shape[1])
    return msg[:, :members], jnp.sum(msg[:, members : members + 3].astype(F32), axis=1)


def update_kernel(got_ref, loc_ref, y_ref, z_ref, w_ref, out_ref, mean_ref):
    parts, ny, nl, nx, members = got_ref.shape
    levels = parts * nl
    part = 16
    rows = part * levels
    step = pl.program_id(0)
    ii = lax.broadcasted_iota(jnp.int32, (rows, rows), 0)
    jj = lax.broadcasted_iota(jnp.int32, (rows, rows), 1)
    order = jnp.where(jj == (ii % levels) * part + ii // levels, 1.0, 0.0).astype(BF)
    blocks, weights = [], []
    for y in range(ny):
        for x in range(0, nx, part):
            block = jnp.concatenate(
                [got_ref[lv // nl, y, lv % nl, x : x + part] for lv in range(levels)], axis=0
            )
            blocks.append(jnp.dot(order, block, preferred_element_type=F32))
        weight = loc_ref[y].astype(F32)
        weight = jnp.broadcast_to(weight[:, None, :], (nx, levels, weight.shape[1]))
        weights.append(weight.reshape(nx * levels, weight.shape[2]))
    block = jnp.concatenate(blocks, axis=0)
    xbar = jnp.sum(block, axis=1, keepdims=True) * (1.0 / members)
    anom = (block - xbar).astype(BF)
    cross = mm(anom, y_ref[...], NT, None) * (1.0 / (members - 1))
    gain = (cross * jnp.concatenate(weights, axis=0)).astype(BF)
    result = anom.astype(F32) - jnp.dot(gain, z_ref[...], preferred_element_type=F32)
    result = result.reshape(ny, nx, levels, members).astype(BF)
    column = xbar + jnp.sum(mm(gain, w_ref[...], NT, None), axis=1, keepdims=True)
    count = nx * levels
    lane = lax.broadcasted_iota(jnp.int32, (count, 128), 1)
    place = lax.broadcasted_iota(jnp.int32, (count, 128), 0) // levels + step * nx

    @pl.when(step == 0)
    def _():
        mean_ref[...] = jnp.zeros_like(mean_ref)

    for y in range(ny):
        out_ref[:, y] = result[y]
        spread = jnp.where(lane == place, column[y * count : (y + 1) * count], 0.0)
        mean_ref[y] += jnp.sum(spread.reshape(nx, levels, 128), axis=0)


def update(got, loc, ybf, zmat, wrows):
    parts, ny, nl, nx, members = got.shape
    n_obs = ybf.shape[0]
    levels = parts * nl
    wide = 32
    out, mean = pl.pallas_call(
        update_kernel,
        out_shape=(
            jax.ShapeDtypeStruct((nx, ny, levels, members), BF),
            jax.ShapeDtypeStruct((ny, levels, nx), F32),
        ),
        grid=(nx // wide,),
        in_specs=[
            pl.BlockSpec((parts, ny, nl, wide, members), lambda i: (0, 0, 0, i, 0)),
            pl.BlockSpec((ny, wide, n_obs), lambda i: (0, i, 0)),
            VM,
            VM,
            VM,
        ],
        out_specs=(
            pl.BlockSpec((wide, ny, levels, members), lambda i: (i, 0, 0, 0)),
            pl.BlockSpec((ny, levels, nx), lambda i: (0, 0, 0)),
        ),
        compiler_params=pltpu.CompilerParams(vmem_limit_bytes=24 << 20),
        cost_estimate=pl.CostEstimate(flops=3 * 10**9, bytes_accessed=5 << 20, transcendentals=0),
    )(got, loc, ybf, zmat, wrows)
    return mean.transpose(2, 0, 1), out


def local(state, obs_col, obs_row, foot_off, obs_lev, obs_val, obs_err, loc):
    nx, ny, nl, members = state.shape
    grid = lax.optimization_barrier(jnp.transpose(state, (1, 2, 0, 3)))
    msg, grid = observe(grid, obs_col, obs_row, foot_off, obs_lev, ny * lax.axis_size("gy"))
    ybf, hbar = share(msg)
    size = lax.axis_size("lev")
    grid, ybf, hbar = lax.optimization_barrier((grid, ybf, hbar))
    got = swap(grid.reshape(size, ny // size, nl, nx, members), "lev")
    zmat, wrows = solve(ybf, obs_val - hbar, obs_err)
    return update(got, jnp.transpose(loc, (1, 0, 2)), ybf, zmat, wrows)


def solution(mesh):
    return jax.shard_map(
        local,
        mesh=mesh,
        in_specs=(
            P("gx", "gy", "lev", None),
            P("gx"),
            P("gx"),
            P("gx", None),
            P("gx"),
            P("gx"),
            P("gx"),
            P("gx", ("gy", "lev"), None),
        ),
        out_specs=(P("gx", ("gy", "lev"), None), P("gx", ("gy", "lev"), None, None)),
        check_vma=False,
    )
```
